32 devices in a mesh: seq: 16 (over z, x, core), head: 2 (over y).
Axes of the slice: x: 2, y: 2, z: 4, core: 2. Of those that a mesh axis runs over, the one named last changes fastest.
Arguments:
- x_proj: bfloat16 [4096, 8192], P(('seq', 'head')), may hold values from -6 to 6
- z_proj: bfloat16 [4096, 8192], P(('seq', 'head')), may hold values from -6 to 6
- b_proj: bfloat16 [4096, 1024], P(('seq', 'head')), may hold values from -6 to 6
- c_proj: bfloat16 [4096, 1024], P(('seq', 'head')), may hold values from -6 to 6
- dt_raw: bfloat16 [4096, 128], P(('seq', 'head')), may hold values from -3.2 to 3.2, as said below
- dt_bias: float32 [128], P('head'), may hold values from -6.3 to -1.2, as said below
- a_log: float32 [128], P('head'), as said below
- d_skip: float32 [128], P('head'), may hold values from 0.5 to 2
- conv_x: float32 [4, 8192], P(None, 'head'), may hold values from -3 to 3
- conv_bias_x: float32 [8192], P('head'), may hold values from -3 to 3
- conv_bc: float32 [4, 2, 1024], P(None, None, 'head'), may hold values from -3 to 3
- conv_bias_bc: float32 [2, 1024], P(None, 'head'), may hold values from -3 to 3
- norm_weight: float32 [8192], P('head'), may hold values from 0.25 to 1.75
- out_weight: bfloat16 [8192, 4096], P('head', 'seq'), may hold values from -0.0625 to 0.0625
Outputs:
- mixed: bfloat16 [4096, 4096], P(('seq', 'head'))
The draws below stay inside these ranges and needn't reach their ends.
Inputs may be any that keep to these rules, and one draw needn't show every extreme that they name: `dt_raw`: A normal draw times 0.7 plus an offset common to each head and each aligned run of 256 tokens. `dt_bias`: the inverse softplus of a per-head step size between 0.002 and 0.25. Finite; exp(a_log) lies above 0.0 and at most 0.3.
All inputs are finite; a program needn't handle non-finite values.
Results may differ from the reference program's by a relative error of at most 0.014.
Values may be sent and summed in bfloat16 or wider, within the bound.
A program may use at most 192 MiB of HBM per device.

```python
import jax
import jax.numpy as jnp
from jax import lax

D = 4096
HEADS = 128
HEAD_DIM = 64
STATE = 128
GROUPS = 8
CONV = 4
TOK_DEV = 256
SPAN = 128
DI = 8192
TOKENS = 4096
N_HEAD = 2


def head_kinds(key):
    order = jax.random.permutation(jax.random.fold_in(key, 101), HEADS)
    return order < HEADS // 2


def draw_dt_bias(key, part):
    slow_heads = head_kinds(key)
    uniform_draw = jax.random.uniform(jax.random.fold_in(key, 102), (HEADS,), jnp.float32)
    lower_log = jnp.where(slow_heads, jnp.log(0.002), jnp.log(0.08))
    upper_log = jnp.where(slow_heads, jnp.log(0.006), jnp.log(0.25))
    step_value = jnp.exp(lower_log + uniform_draw * (upper_log - lower_log))
    return jnp.log(jnp.expm1(step_value)).astype(jnp.float32)


def draw_a_log(key, part):
    slow_heads = head_kinds(key)
    uniform_draw = jax.random.uniform(jax.random.fold_in(key, 105), (HEADS,), jnp.float32)
    slow_log = jnp.log(0.1) + uniform_draw * (jnp.log(0.6) - jnp.log(0.1)) - jnp.log(0.004 * TOKENS)
    fast_log = jnp.log(0.15) + uniform_draw * (jnp.log(0.3) - jnp.log(0.15))
    return jnp.where(slow_heads, slow_log, fast_log).astype(jnp.float32)


def draw_dt_raw(key, part):
    noise_part = jax.random.truncated_normal(jax.random.fold_in(key, 103), -3.0, 3.0, (TOKENS, HEADS), jnp.float32) * 0.7
    offsets = jax.random.uniform(jax.random.fold_in(key, 104), (TOKENS // TOK_DEV, HEADS), jnp.float32, minval=-1.0, maxval=1.0)
    return (noise_part + jnp.repeat(offsets, TOK_DEV, axis=0)).astype(jnp.bfloat16)


def block_levels(own_key, shape, pieces, smallest, high):
    loudness = 1.0
    for axis_at, shards_of in pieces:
        steps = jax.random.uniform(jax.random.fold_in(jax.random.fold_in(own_key, 6), axis_at), (shards_of,), jnp.float32, smallest / len(pieces), high / len(pieces))
        loudness = loudness * jnp.repeat(jnp.exp(steps), shape[axis_at] // shards_of).reshape((-1,) + (1,) * (len(shape) - 1 - axis_at))
    return loudness


def normal_values(stream_key, extent, scale, most, split=(), held_as=jnp.bfloat16):
    gain = block_levels(stream_key, extent, split, -0.22, 0.18) if split else 1.0
    array = jax.random.normal(stream_key, extent, jnp.float32) * scale * gain
    return jnp.minimum(jnp.maximum(array, -most), most).astype(held_as)


def setup_inputs(seed: int = 0) -> dict:
    key_of = jax.random.split(jax.random.key(seed), 15)
    x_proj = normal_values(key_of[0], (TOKENS, DI), 1.0, 6.0, ((0, 32),))
    z_proj = normal_values(key_of[1], (TOKENS, DI), 1.0, 6.0, ((0, 32),))
    b_proj = normal_values(key_of[2], (TOKENS, GROUPS * STATE), 1.0, 6.0, ((0, 32),))
    c_proj = normal_values(key_of[3], (TOKENS, GROUPS * STATE), 1.0, 6.0, ((0, 32),))
    dt_raw = draw_dt_raw(jax.random.fold_in(key_of[14], 71), 0)
    dt_bias = draw_dt_bias(jax.random.fold_in(key_of[14], 71), 0)
    a_log = draw_a_log(jax.random.fold_in(key_of[14], 71), 0)
    d_skip = jnp.clip(0.5 + 1.5 * jax.random.uniform(key_of[7], (HEADS,), jnp.float32) ** block_levels(key_of[7], (HEADS,), ((0, 2),), -0.2, 0.2), 0.5, 2.0)
    conv_x = normal_values(key_of[8], (CONV, DI), CONV ** -0.5, 3.0, ((1, 2),), jnp.float32)
    conv_bias_x = normal_values(key_of[9], (DI,), 0.5, 3.0, ((0, 2),), jnp.float32)
    conv_bc = normal_values(key_of[10], (CONV, 2, GROUPS * STATE), CONV ** -0.5, 3.0, ((2, 2),), jnp.float32)
    conv_bias_bc = normal_values(key_of[11], (2, GROUPS * STATE), 0.5, 3.0, ((1, 2),), jnp.float32)
    norm_weight = jnp.clip(1.0 + 0.15 * jax.random.normal(key_of[12], (DI,), jnp.float32), 0.25, 1.75)
    out_weight = normal_values(key_of[13], (DI, D), DI ** -0.5, 0.0625, ((0, 2), (1, 16)))
    return {"x_proj": x_proj, "z_proj": z_proj, "b_proj": b_proj, "c_proj": c_proj, "dt_raw": dt_raw, "dt_bias": dt_bias, "a_log": a_log, "d_skip": d_skip, "conv_x": conv_x, "conv_bias_x": conv_bias_x, "conv_bc": conv_bc, "conv_bias_bc": conv_bias_bc, "norm_weight": norm_weight, "out_weight": out_weight}


def conv_silu(inputs, weight, bias_row):
    taps = weight.shape[0]
    padded = jnp.pad(inputs.astype(jnp.float32), ((taps - 1, 0), (0, 0)))
    length = inputs.shape[0]
    summed = jnp.broadcast_to(bias_row, inputs.shape).astype(jnp.float32)
    for offset in range(taps):
        summed = summed + weight[offset] * padded[offset:offset + length]
    return jax.nn.silu(summed).astype(jnp.bfloat16)

def to_bf16_f32(value):
    rounded = lax.optimization_barrier(value.astype(jnp.bfloat16))
    return rounded.astype(jnp.float32)

def reference(x_proj, z_proj, b_proj, c_proj, dt_raw, dt_bias, a_log, d_skip, conv_x, conv_bias_x, conv_bc, conv_bias_bc, norm_weight, out_weight):
    high = lax.Precision.HIGHEST
    x_conv = conv_silu(x_proj, conv_x, conv_bias_x)
    b_conv = conv_silu(b_proj, conv_bc[:, 0], conv_bias_bc[0])
    c_conv = conv_silu(c_proj, conv_bc[:, 1], conv_bias_bc[1])
    step_size = jax.nn.softplus(dt_raw.astype(jnp.float32) + dt_bias)
    coeff = -jnp.exp(a_log)
    blocks = TOKENS // SPAN
    per_group = HEADS // GROUPS
    x_blocks = x_conv.reshape(blocks, SPAN, HEADS, HEAD_DIM)
    b_blocks = b_conv.reshape(blocks, SPAN, GROUPS, STATE)
    c_blocks = c_conv.reshape(blocks, SPAN, GROUPS, STATE)
    step_blocks = step_size.reshape(blocks, SPAN, HEADS)
    causal = jnp.arange(SPAN)[:, None] >= jnp.arange(SPAN)[None, :]

    def span_step(state, inputs):
        x_span, b_span, c_span, step_span = inputs
        x_float = x_span.astype(jnp.float32)
        b_float = b_span.astype(jnp.float32)
        c_float = c_span.astype(jnp.float32)
        cumulative = jnp.cumsum(coeff * step_span, axis=0)
        scores = jnp.einsum('tgn,sgn->gts', c_float, b_float, precision=high)
        by_head = cumulative.T
        spread = by_head[:, :, None] - by_head[:, None, :]
        decays = jnp.exp(jnp.where(causal, spread, -jnp.inf))
        scaled = decays * step_span.T[:, None, :]
        mix_weights = (scaled.reshape(GROUPS, per_group, SPAN, SPAN) * scores[:, None]).reshape(HEADS, SPAN, SPAN)
        mix_weights = to_bf16_f32(mix_weights)
        y_local = jnp.einsum('hts,shp->thp', mix_weights, x_float, precision=high)
        state_scale = step_span * jnp.exp(cumulative[-1:] - cumulative)
        x_weighted = to_bf16_f32(x_float * state_scale[:, :, None])
        piece = jnp.einsum('sgqp,sgn->gqpn', x_weighted.reshape(SPAN, GROUPS, per_group, HEAD_DIM), b_float, precision=high)
        piece = piece.reshape(HEADS, HEAD_DIM, STATE)
        start_state = to_bf16_f32(state).reshape(GROUPS, per_group, HEAD_DIM, STATE)
        y_carry = jnp.einsum('tgn,gqpn->tgqp', c_float, start_state, precision=high).reshape(SPAN, HEADS, HEAD_DIM)
        y_carry = y_carry * jnp.exp(cumulative)[:, :, None]
        outputs = y_local + y_carry + d_skip[:, None] * x_float
        new_state = jnp.exp(cumulative[-1])[:, None, None] * state + piece
        return (new_state, outputs)
    initial = jnp.zeros((HEADS, HEAD_DIM, STATE), jnp.float32)
    final_state, outputs = lax.scan(span_step, initial, (x_blocks, b_blocks, c_blocks, step_blocks))
    outputs = outputs.reshape(TOKENS, DI)
    gated = outputs * jax.nn.silu(z_proj.astype(jnp.float32))
    grouped = gated.reshape(TOKENS, GROUPS, DI // GROUPS)
    normed = grouped / jnp.sqrt(lax.optimization_barrier(jnp.mean(grouped * grouped, axis=-1, keepdims=True)) + 1.0)
    normed = (normed.reshape(TOKENS, DI) * norm_weight).astype(jnp.bfloat16)
    block_rows = DI // N_HEAD
    summed = jnp.zeros((TOKENS, D), jnp.float32)
    for block_idx in range(N_HEAD):
        rows_lo = block_idx * block_rows
        partial_sum = jnp.dot(normed[:, rows_lo:rows_lo + block_rows], out_weight[rows_lo:rows_lo + block_rows], preferred_element_type=jnp.float32)
        summed = summed + to_bf16_f32(partial_sum)
    return summed.astype(jnp.bfloat16)
```

```python
import jax
import jax.numpy as jnp
from jax import lax
from jax.sharding import PartitionSpec as P

HEAD_DIM = 64
STATE = 128
GROUPS = 8
SPAN = 128
DI = 8192


def from_behind(array, axis, by):
    count = lax.axis_size(axis)
    pairs = [(i, i + by) for i in range(count) if 0 <= i + by < count]
    return lax.ppermute(array, axis, pairs)


def carry_in(log_total, final_state, axis):
    count, mine = (lax.axis_size(axis), lax.axis_index(axis))
    width = final_state.shape[-1]
    flat = final_state.reshape(count, -1, width).astype(jnp.bfloat16)
    rows = flat.shape[1]
    pieces = lax.all_to_all(flat, axis, split_axis=0, concat_axis=0)
    logs = lax.all_gather(log_total, axis)
    by_row = jnp.repeat(logs, final_state.shape[1], axis=1)
    decays = jnp.exp(lax.dynamic_slice_in_dim(by_row, mine * rows, rows, axis=1))
    running = jnp.zeros((rows, width), jnp.float32)
    starts = []
    for position in range(count):
        starts.append(running.astype(jnp.bfloat16))
        running = decays[position][:, None] * running + pieces[position].astype(jnp.float32)
    back = lax.all_to_all(jnp.stack(starts), axis, split_axis=0, concat_axis=0)
    return back.reshape(final_state.shape).astype(jnp.float32)


def depthwise(current, previous, weight, bias_row):
    padded = jnp.concatenate([previous, current], axis=0).astype(jnp.float32)
    token_count = current.shape[0]
    summed = jnp.broadcast_to(bias_row, current.shape)
    for offset in range(weight.shape[0]):
        summed = summed + weight[offset] * padded[offset : offset + token_count]
    return jax.nn.silu(summed).astype(jnp.bfloat16)


def block_weights(c_blocks, b_blocks, cumulative, step_size, per_group):
    scores = jnp.einsum("ktgn,ksgn->kgts", c_blocks, b_blocks, preferred_element_type=jnp.float32)
    by_head = jnp.transpose(cumulative, (0, 2, 1))
    spread = by_head[:, :, :, None] - by_head[:, :, None, :]
    length = cumulative.shape[1]
    causal = jnp.arange(length)[:, None] >= jnp.arange(length)[None, :]
    decays = jnp.exp(jnp.where(causal, spread, -jnp.inf))
    scaled = decays * jnp.transpose(step_size, (0, 2, 1))[:, :, None, :]
    block_count = cumulative.shape[0]
    head_count = cumulative.shape[2]
    grouped = scaled.reshape(block_count, -1, per_group, length, length) * scores[:, :, None]
    return grouped.reshape(block_count, head_count, length, length).astype(jnp.bfloat16)


def per_device(
    x_proj,
    z_proj,
    b_proj,
    c_proj,
    dt_raw,
    dt_bias,
    a_log,
    d_skip,
    conv_x,
    conv_bias_x,
    conv_bc,
    conv_bias_bc,
    norm_weight,
    out_weight,
):
    x_heads, z_heads, b_heads, c_heads, dt_heads = (
        lax.all_to_all(x_proj, "head", split_axis=1, concat_axis=0, tiled=True),
        lax.all_to_all(z_proj, "head", split_axis=1, concat_axis=0, tiled=True),
        lax.all_to_all(b_proj, "head", split_axis=1, concat_axis=0, tiled=True),
        lax.all_to_all(c_proj, "head", split_axis=1, concat_axis=0, tiled=True),
        lax.all_to_all(dt_raw, "head", split_axis=1, concat_axis=0, tiled=True),
    )
    kernel_len = conv_x.shape[0]
    x_cols = x_heads.shape[1]
    bc_cols = b_heads.shape[1]
    last_rows = jnp.concatenate(
        [x_heads[-(kernel_len - 1) :], b_heads[-(kernel_len - 1) :], c_heads[-(kernel_len - 1) :]],
        axis=1,
    )
    before = from_behind(last_rows, "seq", 1)
    x_conv = depthwise(x_heads, before[:, :x_cols], conv_x, conv_bias_x)
    b_conv = depthwise(
        b_heads, before[:, x_cols : x_cols + bc_cols], conv_bc[:, 0], conv_bias_bc[0]
    )
    c_conv = depthwise(c_heads, before[:, x_cols + bc_cols :], conv_bc[:, 1], conv_bias_bc[1])
    token_count = x_conv.shape[0]
    local_heads = dt_bias.shape[0]
    local_groups = bc_cols // STATE
    per_group = local_heads // local_groups
    blocks = token_count // SPAN
    x_blocks = x_conv.reshape(blocks, SPAN, local_heads, HEAD_DIM)
    b_blocks = b_conv.reshape(blocks, SPAN, local_groups, STATE)
    c_blocks = c_conv.reshape(blocks, SPAN, local_groups, STATE)
    step_size = jax.nn.softplus(dt_heads.astype(jnp.float32) + dt_bias).reshape(
        blocks, SPAN, local_heads
    )
    cumulative = jnp.cumsum(-jnp.exp(a_log) * step_size, axis=1)
    mix_weights = block_weights(c_blocks, b_blocks, cumulative, step_size, per_group)
    y_local = jnp.einsum(
        "khts,kshp->kthp", mix_weights, x_blocks, preferred_element_type=jnp.float32
    )
    state_scale = step_size * jnp.exp(cumulative[:, -1:, :] - cumulative)
    x_weighted = (x_blocks.astype(jnp.float32) * state_scale[:, :, :, None]).astype(jnp.bfloat16)
    x_grouped = x_weighted.reshape(blocks, SPAN, local_groups, per_group, HEAD_DIM)
    pieces = jnp.einsum(
        "ksgqp,ksgn->kgqpn", x_grouped, b_blocks, preferred_element_type=jnp.float32
    )
    pieces = pieces.reshape(blocks, local_heads, HEAD_DIM, STATE)
    totals = cumulative[:, -1, :]
    final_state = jnp.zeros((local_heads, HEAD_DIM, STATE), jnp.float32)
    for block_idx in range(blocks):
        final_state = jnp.exp(totals[block_idx])[:, None, None] * final_state + pieces[block_idx]
    log_total = jnp.sum(totals, axis=0)
    running = carry_in(log_total, final_state, "seq")
    start_list = []
    for block_idx in range(blocks):
        start_list.append(running.astype(jnp.bfloat16))
        running = jnp.exp(totals[block_idx])[:, None, None] * running + pieces[block_idx]
    start_states = jnp.stack(start_list).reshape(blocks, local_groups, per_group, HEAD_DIM, STATE)
    y_carry = jnp.einsum(
        "ktgn,kgqpn->ktgqp", c_blocks, start_states, preferred_element_type=jnp.float32
    )
    y_carry = (
        y_carry.reshape(blocks, SPAN, local_heads, HEAD_DIM) * jnp.exp(cumulative)[:, :, :, None]
    )
    outputs = y_local + y_carry + d_skip[:, None] * x_blocks.astype(jnp.float32)
    outputs = outputs.reshape(token_count, local_heads * HEAD_DIM)
    gated = outputs * jax.nn.silu(z_heads.astype(jnp.float32))
    grouped = gated.reshape(token_count, -1, DI // GROUPS)
    normed = grouped / jnp.sqrt(jnp.mean(grouped * grouped, axis=-1, keepdims=True) + 1.0)
    normed = (normed.reshape(token_count, -1) * norm_weight).astype(jnp.bfloat16)
    terms = jnp.dot(
        normed,
        lax.all_gather(out_weight, "seq", axis=1, tiled=True),
        preferred_element_type=jnp.float32,
    )
    mixed = lax.psum_scatter(terms.astype(jnp.bfloat16), "head", scatter_dimension=0, tiled=True)
    return mixed


def solution(mesh):
    in_specs = (
        P(("seq", "head"), None),
        P(("seq", "head"), None),
        P(("seq", "head"), None),
        P(("seq", "head"), None),
        P(("seq", "head"), None),
        P("head"),
        P("head"),
        P("head"),
        P(None, "head"),
        P("head"),
        P(None, None, "head"),
        P(None, "head"),
        P("head"),
        P("head", "seq"),
    )
    out_specs = P(("seq", "head"), None)
    return jax.shard_map(
        per_device, mesh=mesh, in_specs=in_specs, out_specs=out_specs, check_vma=False
    )
```

```python
import functools

import jax
import jax.numpy as jnp
from jax import lax
from jax.experimental import pallas as pl
from jax.experimental.pallas import tpu as pltpu
from jax.sharding import PartitionSpec as P

HEAD_DIM = 64
STATE = 128
GROUPS = 8
SPAN = 128
DI = 8192
HALO = 16
NT = (((1,), (1,)), ((), ()))


def entry_kernel(count, heads, *refs):
    x_in, z_in, b_in, c_in, dt_in = refs[:5]
    x_out, z_out, b_out, c_out, dt_out, x_halo, b_halo, c_halo = refs[5:13]
    send_sems, recv_sems, local_sems, halo_send, halo_recv = refs[13:]
    seq = lax.axis_index("seq")
    head = lax.axis_index("head")
    rows = x_in.shape[0]
    barrier = pltpu.get_barrier_semaphore()
    last_head = head == heads - 1
    gives_halo = jnp.logical_and(last_head, seq < count - 1)
    takes_halo = seq > 0
    for step in range(1, heads):
        peer = lax.rem(head + step, heads)
        pl.semaphore_signal(
            barrier, inc=1, device_id=(seq, peer), device_id_type=pl.DeviceIdType.MESH
        )

    @pl.when(takes_halo)
    def _():
        pl.semaphore_signal(
            barrier,
            inc=1,
            device_id=(seq - 1, heads - 1),
            device_id_type=pl.DeviceIdType.MESH,
        )

    pl.semaphore_wait(barrier, heads - 1 + jnp.where(gives_halo, heads, 0))

    def columns(ref, width, which):
        return ref.at[:, pl.ds(pl.multiple_of(which * width, 128), width)]

    mine = pl.ds(pl.multiple_of(head * rows, 16), rows)
    plan = (
        (b_in, b_out, True),
        (c_in, c_out, True),
        (dt_in, dt_out, False),
        (x_in, x_out, True),
        (z_in, z_out, True),
    )
    halos = ((x_in, x_halo), (b_in, b_halo), (c_in, c_halo))

    def halo_copy(index, peer):
        source, target = halos[index]
        width = target.shape[1]
        return pltpu.make_async_remote_copy(
            src_ref=source.at[pl.ds(rows - HALO, HALO), pl.ds(peer * width, width)],
            dst_ref=target,
            send_sem=halo_send.at[index, peer],
            recv_sem=halo_recv.at[index],
            device_id=(seq + 1, peer),
            device_id_type=pl.DeviceIdType.MESH,
        )

    @pl.when(gives_halo)
    def _():
        for index in range(len(halos)):
            for peer in range(heads):
                halo_copy(index, peer).start()

    copies = []
    for step in range(1, heads):
        peer = lax.rem(head + step, heads)
        for index, (source, target, split) in enumerate(plan):
            view = columns(source, target.shape[1], peer) if split else source
            copy = pltpu.make_async_remote_copy(
                src_ref=view,
                dst_ref=target.at[mine],
                send_sem=send_sems.at[index, step],
                recv_sem=recv_sems.at[index, step],
                device_id=(seq, peer),
                device_id_type=pl.DeviceIdType.MESH,
            )
            copy.start()
            copies.append(copy)
    for index, (source, target, split) in enumerate(plan):
        view = columns(source, target.shape[1], head) if split else source
        copy = pltpu.make_async_copy(view, target.at[mine], local_sems.at[index])
        copy.start()
        copies.append(copy)

    @pl.when(jnp.logical_not(takes_halo))
    def _():
        for _, target in halos:
            target[...] = jnp.zeros_like(target)

    @pl.when(takes_halo)
    def _():
        for index, (source, target) in enumerate(halos):
            pltpu.make_async_remote_copy(
                src_ref=source.at[pl.ds(rows - HALO, HALO), pl.ds(0, target.shape[1])],
                dst_ref=target,
                send_sem=halo_send.at[index, 0],
                recv_sem=halo_recv.at[index],
                device_id=(seq, head),
                device_id_type=pl.DeviceIdType.MESH,
            ).wait_recv()

    @pl.when(gives_halo)
    def _():
        for index in range(len(halos)):
            for peer in range(heads):
                halo_copy(index, peer).wait_send()

    for copy in copies:
        copy.wait()


def entry_exchange(x_proj, z_proj, b_proj, c_proj, dt_raw):
    count = lax.axis_size("seq")
    heads = lax.axis_size("head")
    rows = x_proj.shape[0] * heads
    x_cols = x_proj.shape[1] // heads
    bc_cols = b_proj.shape[1] // heads
    dtype = x_proj.dtype
    shapes = [
        (rows, x_cols),
        (rows, x_cols),
        (rows, bc_cols),
        (rows, bc_cols),
        (rows, dt_raw.shape[1]),
        (HALO, x_cols),
        (HALO, bc_cols),
        (HALO, bc_cols),
    ]
    return pl.pallas_call(
        functools.partial(entry_kernel, count, heads),
        out_shape=[jax.ShapeDtypeStruct(shape, dtype) for shape in shapes],
        in_specs=[pl.BlockSpec(memory_space=pl.ANY)] * 5,
        out_specs=[pl.BlockSpec(memory_space=pl.ANY)] * 5
        + [pl.BlockSpec(memory_space=pltpu.VMEM)] * 3,
        scratch_shapes=[
            pltpu.SemaphoreType.DMA((5, heads)),
            pltpu.SemaphoreType.DMA((5, heads)),
            pltpu.SemaphoreType.DMA((5,)),
            pltpu.SemaphoreType.DMA((3, heads)),
            pltpu.SemaphoreType.DMA((3,)),
        ],
        compiler_params=pltpu.CompilerParams(collective_id=0, has_side_effects=True),
        name="entry_exchange",
    )(x_proj, z_proj, b_proj, c_proj, dt_raw)


def conv_silu(value_ref, halo_ref, taps_ref, bias_ref, padded):
    tokens = value_ref.shape[0]
    taps = taps_ref.shape[0]
    padded[0:8, :] = halo_ref[HALO - 8 : HALO, :].astype(jnp.float32)
    padded[8 : 8 + tokens, :] = value_ref[...].astype(jnp.float32)
    total = bias_ref[...] + jnp.zeros(value_ref.shape, jnp.float32)
    for offset in range(taps):
        low = 8 - (taps - 1) + offset
        total = total + taps_ref[offset : offset + 1, :] * padded[low : low + tokens, :]
    return (total / (1.0 + jnp.exp(-total))).astype(jnp.bfloat16)


def local_kernel(
    x_ref,
    b_ref,
    c_ref,
    x_halo,
    b_halo,
    c_halo,
    x_taps,
    x_bias,
    b_taps,
    b_bias,
    c_taps,
    c_bias,
    step_t,
    cum_t,
    cum_c,
    skip_ref,
    y_ref,
    piece_ref,
    final_ref,
    c_out,
    x_pad,
    bc_pad,
    x_t,
    x_w,
    final,
):
    tokens, width = x_ref.shape
    heads = step_t.shape[0]
    blocks = tokens // SPAN
    x_conv = conv_silu(x_ref, x_halo, x_taps, x_bias, x_pad)
    b_conv = conv_silu(b_ref, b_halo, b_taps, b_bias, bc_pad)
    c_conv = conv_silu(c_ref, c_halo, c_taps, c_bias, bc_pad)
    c_out[...] = c_conv
    later = lax.broadcasted_iota(jnp.int32, (SPAN, SPAN), 0)
    earlier = lax.broadcasted_iota(jnp.int32, (SPAN, SPAN), 1)
    causal = later >= earlier
    for block in range(blocks):
        low = block * SPAN
        b_blk = b_conv[low : low + SPAN]
        c_blk = c_conv[low : low + SPAN]
        x_t[...] = x_conv[low : low + SPAN].astype(jnp.float32).T
        scores = lax.dot_general(c_blk, b_blk, NT, preferred_element_type=jnp.float32)
        for head in range(heads):
            rows = pl.ds(head * HEAD_DIM, HEAD_DIM)
            column = cum_c[0, low : low + SPAN, head : head + 1]
            row = cum_t[head : head + 1, low : low + SPAN]
            step = step_t[head : head + 1, low : low + SPAN]
            total = row[:, SPAN - 1 : SPAN]
            decays = jnp.exp(jnp.where(causal, column - row, -jnp.inf))
            mix = (decays * step * scores).astype(jnp.bfloat16)
            x_head = x_t[rows, :]
            product = lax.dot_general(
                x_head.astype(jnp.bfloat16), mix, NT, preferred_element_type=jnp.float32
            )
            y_ref[block, rows, :] = product + skip_ref[0, head : head + 1, :] * x_head
            x_w[rows, :] = (x_head * (step * jnp.exp(total - row))).astype(jnp.bfloat16)
        piece = jnp.dot(x_w[...], b_blk, preferred_element_type=jnp.float32)
        piece_ref[block] = piece
        if block == 0:
            final[...] = piece
        else:
            for head in range(heads):
                rows = pl.ds(head * HEAD_DIM, HEAD_DIM)
                decay = jnp.exp(cum_t[head : head + 1, low + SPAN - 1 : low + SPAN])
                final[rows, :] = decay * final[rows, :] + piece_ref[block, rows, :]
    final_ref[...] = final[...].astype(jnp.bfloat16)


def local_scan(x, b, c, halos, x_taps, x_bias, bc_taps, bc_bias, step_t, cum_t, cum_c, skip):
    tokens, x_cols = x.shape
    groups = b.shape[1] // STATE
    width = x_cols // groups
    heads = width // HEAD_DIM
    blocks = tokens // SPAN
    taps = x_taps.shape[0]

    def cols(rows, size):
        return pl.BlockSpec((rows, size), lambda g: (0, g))

    in_specs = [
        cols(tokens, width),
        cols(tokens, STATE),
        cols(tokens, STATE),
        cols(HALO, width),
        cols(HALO, STATE),
        cols(HALO, STATE),
        cols(taps, width),
        cols(1, width),
        cols(taps, STATE),
        cols(1, STATE),
        cols(taps, STATE),
        cols(1, STATE),
        pl.BlockSpec((heads, tokens), lambda g: (g, 0)),
        pl.BlockSpec((heads, tokens), lambda g: (g, 0)),
        pl.BlockSpec((1, tokens, heads), lambda g: (g, 0, 0)),
        pl.BlockSpec((1, heads, 1), lambda g: (g, 0, 0)),
    ]
    out_specs = [
        pl.BlockSpec((blocks, width, SPAN), lambda g: (0, g, 0)),
        pl.BlockSpec((blocks, width, STATE), lambda g: (0, g, 0)),
        pl.BlockSpec((width, STATE), lambda g: (g, 0)),
        cols(tokens, STATE),
    ]
    out_shape = [
        jax.ShapeDtypeStruct((blocks, x_cols, SPAN), jnp.float32),
        jax.ShapeDtypeStruct((blocks, x_cols, STATE), jnp.float32),
        jax.ShapeDtypeStruct((x_cols, STATE), jnp.bfloat16),
        jax.ShapeDtypeStruct((tokens, groups * STATE), jnp.bfloat16),
    ]
    return pl.pallas_call(
        local_kernel,
        grid=(groups,),
        in_specs=in_specs,
        out_specs=out_specs,
        out_shape=out_shape,
        scratch_shapes=[
            pltpu.VMEM((tokens + 8, width), jnp.float32),
            pltpu.VMEM((tokens + 8, STATE), jnp.float32),
            pltpu.VMEM((width, SPAN), jnp.float32),
            pltpu.VMEM((width, SPAN), jnp.bfloat16),
            pltpu.VMEM((width, STATE), jnp.float32),
        ],
        compiler_params=pltpu.CompilerParams(dimension_semantics=("arbitrary",)),
        cost_estimate=pl.CostEstimate(
            flops=20000000000, bytes_accessed=16000000, transcendentals=4000000
        ),
        name="local_scan",
    )(
        x,
        b,
        c,
        *halos,
        x_taps,
        x_bias[None],
        bc_taps[:, 0],
        bc_bias[0:1],
        bc_taps[:, 1],
        bc_bias[1:2],
        step_t,
        cum_t,
        cum_c,
        skip,
    )


def carry_kernel(start_ref, piece_ref, c_ref, cum_t, y_ref, z_ref, gain_ref, out_ref, running, y_t):
    tokens, width = z_ref.shape
    heads = cum_t.shape[0]
    blocks = tokens // SPAN
    running[...] = start_ref[...].astype(jnp.float32)
    for block in range(blocks):
        low = block * SPAN
        c_blk = c_ref[low : low + SPAN, :]
        carried = lax.dot_general(
            running[...].astype(jnp.bfloat16), c_blk, NT, preferred_element_type=jnp.float32
        )
        y_t[...] = carried
        for head in range(heads):
            rows = pl.ds(head * HEAD_DIM, HEAD_DIM)
            row = jnp.exp(cum_t[head : head + 1, low : low + SPAN])
            y_t[rows, :] = y_ref[block, rows, :] + y_t[rows, :] * row
            if block < blocks - 1:
                running[rows, :] = (
                    row[:, SPAN - 1 : SPAN] * running[rows, :] + piece_ref[block, rows, :]
                )
        gate = z_ref[low : low + SPAN, :].astype(jnp.float32)
        gated = y_t[...].T * (gate / (1.0 + jnp.exp(-gate)))
        mean = jnp.sum(gated * gated, axis=-1, keepdims=True) * (1.0 / width)
        normed = gated * lax.rsqrt(mean + 1.0)
        out_ref[low : low + SPAN, :] = (normed * gain_ref[...]).astype(jnp.bfloat16)


def carry_norm(start, pieces, c_conv, cum_t, y_t, z, gain):
    tokens, x_cols = z.shape
    groups = c_conv.shape[1] // STATE
    width = x_cols // groups
    heads = width // HEAD_DIM
    blocks = tokens // SPAN
    return pl.pallas_call(
        carry_kernel,
        grid=(groups,),
        in_specs=[
            pl.BlockSpec((width, STATE), lambda g: (g, 0)),
            pl.BlockSpec((blocks, width, STATE), lambda g: (0, g, 0)),
            pl.BlockSpec((tokens, STATE), lambda g: (0, g)),
            pl.BlockSpec((heads, tokens), lambda g: (g, 0)),
            pl.BlockSpec((blocks, width, SPAN), lambda g: (0, g, 0)),
            pl.BlockSpec((tokens, width), lambda g: (0, g)),
            pl.BlockSpec((1, width), lambda g: (0, g)),
        ],
        out_specs=pl.BlockSpec((tokens, width), lambda g: (0, g)),
        out_shape=jax.ShapeDtypeStruct((tokens, x_cols), jnp.bfloat16),
        scratch_shapes=[
            pltpu.VMEM((width, STATE), jnp.float32),
            pltpu.VMEM((width, SPAN), jnp.float32),
        ],
        compiler_params=pltpu.CompilerParams(dimension_semantics=("arbitrary",)),
        cost_estimate=pl.CostEstimate(
            flops=5000000000, bytes_accessed=14000000, transcendentals=1000000
        ),
        name="carry_norm",
    )(start, pieces, c_conv, cum_t, y_t, z, gain[None])


def prefix_kernel(count, final_ref, logs_ref, out_ref, pieces, logs, starts, *sems):
    piece_send, piece_recv, log_send, log_recv, start_send, start_recv, own = sems
    seq = lax.axis_index("seq")
    head = lax.axis_index("head")
    rows = pieces.shape[1]
    barrier = pltpu.get_barrier_semaphore()

    def peer_of(step):
        return lax.rem(seq + step, count)

    def part(which):
        return pl.ds(pl.multiple_of(which * rows, 16), rows)

    def remote(source, target, send, recv, peer):
        return pltpu.make_async_remote_copy(
            src_ref=source,
            dst_ref=target,
            send_sem=send,
            recv_sem=recv,
            device_id=(peer, head),
            device_id_type=pl.DeviceIdType.MESH,
        )

    def log_copy(step):
        return remote(
            logs_ref, logs.at[seq], log_send.at[step], log_recv.at[step], peer_of(step)
        )

    def piece_copy(step):
        return remote(
            final_ref.at[part(peer_of(step))],
            pieces.at[seq],
            piece_send.at[step],
            piece_recv.at[step],
            peer_of(step),
        )

    def start_copy(step):
        return remote(
            starts.at[peer_of(step)],
            out_ref.at[part(seq)],
            start_send.at[step],
            start_recv.at[step],
            peer_of(step),
        )

    def each(body):
        def lap(step, carry):
            body(step)
            return carry

        lax.fori_loop(1, count, lap, 0)

    def greet(step):
        pl.semaphore_signal(
            barrier, inc=1, device_id=(peer_of(step), head), device_id_type=pl.DeviceIdType.MESH
        )

    each(greet)
    pl.semaphore_wait(barrier, count - 1)

    def send(step):
        log_copy(step).start()
        piece_copy(step).start()

    each(send)
    own_piece = pltpu.make_async_copy(final_ref.at[part(seq)], pieces.at[seq], own.at[0])
    own_log = pltpu.make_async_copy(logs_ref, logs.at[seq], own.at[1])
    own_piece.start()
    own_log.start()
    own_piece.wait()
    own_log.wait()

    def land(step):
        log_copy(step).wait()
        piece_copy(step).wait()

    each(land)
    per_head = min(rows, HEAD_DIM)
    first = seq * rows // HEAD_DIM
    lanes = logs.shape[2]

    def scan(position, running):
        for index in range(rows // per_head):
            low = index * per_head
            starts[position, low : low + per_head, :] = running[index].astype(jnp.bfloat16)
        decays = jnp.exp(pltpu.roll(logs[position], lax.rem(lanes - first, lanes), 1))
        following = []
        for index in range(rows // per_head):
            low = index * per_head
            piece = pieces[position, low : low + per_head, :].astype(jnp.float32)
            following.append(decays[0:1, index : index + 1] * running[index] + piece)
        return tuple(following)

    zero = jnp.zeros((per_head, pieces.shape[2]), jnp.float32)
    lax.fori_loop(0, count, scan, (zero,) * (rows // per_head))
    each(lambda step: start_copy(step).start())
    own_start = pltpu.make_async_copy(starts.at[seq], out_ref.at[part(seq)], own.at[0])
    own_start.start()
    own_start.wait()
    each(lambda step: start_copy(step).wait())


def carry_in(log_total, final_state):
    count = lax.axis_size("seq")
    total, width = final_state.shape
    rows = total // count
    logs = jnp.broadcast_to(jnp.pad(log_total, (0, 128 - log_total.shape[0]))[None], (8, 128))
    vmem = pl.BlockSpec(memory_space=pltpu.VMEM)
    dma = pltpu.SemaphoreType.DMA
    return pl.pallas_call(
        functools.partial(prefix_kernel, count),
        out_shape=jax.ShapeDtypeStruct(final_state.shape, final_state.dtype),
        in_specs=[vmem, vmem],
        out_specs=vmem,
        scratch_shapes=[
            pltpu.VMEM((count, rows, width), jnp.bfloat16),
            pltpu.VMEM((count, 8, 128), jnp.float32),
            pltpu.VMEM((count, rows, width), jnp.bfloat16),
            dma((count,)),
            dma((count,)),
            dma((count,)),
            dma((count,)),
            dma((count,)),
            dma((count,)),
            dma((2,)),
        ],
        compiler_params=pltpu.CompilerParams(collective_id=1, has_side_effects=True),
        name="prefix_exchange",
    )(final_state, logs)


def per_device(
    x_proj,
    z_proj,
    b_proj,
    c_proj,
    dt_raw,
    dt_bias,
    a_log,
    d_skip,
    conv_x,
    conv_bias_x,
    conv_bc,
    conv_bias_bc,
    norm_weight,
    out_weight,
):
    x_heads, z_heads, b_heads, c_heads, dt_full, *halos = entry_exchange(
        x_proj, z_proj, b_proj, c_proj, dt_raw
    )
    token_count = x_heads.shape[0]
    local_heads = dt_bias.shape[0]
    local_groups = b_heads.shape[1] // STATE
    per_group = local_heads // local_groups
    blocks = token_count // SPAN
    dt_heads = lax.dynamic_slice_in_dim(
        dt_full, lax.axis_index("head") * local_heads, local_heads, axis=1
    )
    step_size = jax.nn.softplus(dt_heads.astype(jnp.float32) + dt_bias)
    rate = (-jnp.exp(a_log) * step_size).reshape(blocks, SPAN, local_heads)
    cumulative = jnp.cumsum(rate, axis=1)
    log_total = jnp.sum(cumulative[:, -1], axis=0)
    cumulative = cumulative.reshape(token_count, local_heads)
    step_t = step_size.T
    cum_t = cumulative.T
    cum_c = jnp.transpose(
        cumulative.reshape(token_count, local_groups, per_group), (1, 0, 2)
    )
    y_t, pieces, final_state, c_conv = local_scan(
        x_heads,
        b_heads,
        c_heads,
        halos,
        conv_x,
        conv_bias_x,
        conv_bc,
        conv_bias_bc,
        step_t,
        cum_t,
        cum_c,
        d_skip.reshape(local_groups, per_group, 1),
    )
    start = carry_in(log_total, final_state)
    normed = carry_norm(start, pieces, c_conv, cum_t, y_t, z_heads, norm_weight)
    terms = jnp.dot(
        normed,
        lax.all_gather(out_weight, "seq", axis=1, tiled=True),
        preferred_element_type=jnp.float32,
    )
    return lax.psum_scatter(terms.astype(jnp.bfloat16), "head", scatter_dimension=0, tiled=True)


def solution(mesh):
    in_specs = (
        P(("seq", "head"), None),
        P(("seq", "head"), None),
        P(("seq", "head"), None),
        P(("seq", "head"), None),
        P(("seq", "head"), None),
        P("head"),
        P("head"),
        P("head"),
        P(None, "head"),
        P("head"),
        P(None, None, "head"),
        P(None, "head"),
        P("head"),
        P("head", "seq"),
    )
    out_specs = P(("seq", "head"), None)
    return jax.shard_map(
        per_device, mesh=mesh, in_specs=in_specs, out_specs=out_specs, check_vma=False
    )
```

```python
import functools

import jax
import jax.numpy as jnp
from jax import lax
from jax.experimental import pallas as pl
from jax.experimental.pallas import tpu as pltpu
from jax.sharding import PartitionSpec as P

HEAD_DIM = 64
STATE = 128
GROUPS = 8
SPAN = 128
DI = 8192
HALO = 16
NT = (((1,), (1,)), ((), ()))


def entry_kernel(count, heads, *refs):
    x_in, z_in, b_in, c_in, dt_in = refs[:5]
    x_out, z_out, b_out, c_out, dt_out, x_halo, b_halo, c_halo = refs[5:13]
    send_sems, recv_sems, local_sems, halo_send, halo_recv = refs[13:]
    seq = lax.axis_index("seq")
    head = lax.axis_index("head")
    rows = x_in.shape[0]
    barrier = pltpu.get_barrier_semaphore()
    last_head = head == heads - 1
    gives_halo = jnp.logical_and(last_head, seq < count - 1)
    takes_halo = seq > 0
    for step in range(1, heads):
        peer = lax.rem(head + step, heads)
        pl.semaphore_signal(
            barrier, inc=1, device_id=(seq, peer), device_id_type=pl.DeviceIdType.MESH
        )

    @pl.when(takes_halo)
    def _():
        pl.semaphore_signal(
            barrier,
            inc=1,
            device_id=(seq - 1, heads - 1),
            device_id_type=pl.DeviceIdType.MESH,
        )

    pl.semaphore_wait(barrier, heads - 1 + jnp.where(gives_halo, heads, 0))

    def columns(ref, width, which):
        return ref.at[:, pl.ds(pl.multiple_of(which * width, 128), width)]

    mine = pl.ds(pl.multiple_of(head * rows, 16), rows)
    plan = (
        (b_in, b_out, True),
        (c_in, c_out, True),
        (dt_in, dt_out, False),
        (x_in, x_out, True),
        (z_in, z_out, True),
    )
    halos = ((x_in, x_halo), (b_in, b_halo), (c_in, c_halo))

    def halo_copy(index, peer):
        source, target = halos[index]
        width = target.shape[1]
        return pltpu.make_async_remote_copy(
            src_ref=source.at[pl.ds(rows - HALO, HALO), pl.ds(peer * width, width)],
            dst_ref=target,
            send_sem=halo_send.at[index, peer],
            recv_sem=halo_recv.at[index],
            device_id=(seq + 1, peer),
            device_id_type=pl.DeviceIdType.MESH,
        )

    @pl.when(gives_halo)
    def _():
        for index in range(len(halos)):
            for peer in range(heads):
                halo_copy(index, peer).start()

    copies = []
    for step in range(1, heads):
        peer = lax.rem(head + step, heads)
        for index, (source, target, split) in enumerate(plan):
            view = columns(source, target.shape[1], peer) if split else source
            copy = pltpu.make_async_remote_copy(
                src_ref=view,
                dst_ref=target.at[mine],
                send_sem=send_sems.at[index, step],
                recv_sem=recv_sems.at[index, step],
                device_id=(seq, peer),
                device_id_type=pl.DeviceIdType.MESH,
            )
            copy.start()
            copies.append(copy)
    for index, (source, target, split) in enumerate(plan):
        view = columns(source, target.shape[1], head) if split else source
        copy = pltpu.make_async_copy(view, target.at[mine], local_sems.at[index])
        copy.start()
        copies.append(copy)

    @pl.when(jnp.logical_not(takes_halo))
    def _():
        for _, target in halos:
            target[...] = jnp.zeros_like(target)

    @pl.when(takes_halo)
    def _():
        for index, (source, target) in enumerate(halos):
            pltpu.make_async_remote_copy(
                src_ref=source.at[pl.ds(rows - HALO, HALO), pl.ds(0, target.shape[1])],
                dst_ref=target,
                send_sem=halo_send.at[index, 0],
                recv_sem=halo_recv.at[index],
                device_id=(seq, head),
                device_id_type=pl.DeviceIdType.MESH,
            ).wait_recv()

    @pl.when(gives_halo)
    def _():
        for index in range(len(halos)):
            for peer in range(heads):
                halo_copy(index, peer).wait_send()

    for copy in copies:
        copy.wait()


def entry_exchange(x_proj, z_proj, b_proj, c_proj, dt_raw):
    count = lax.axis_size("seq")
    heads = lax.axis_size("head")
    rows = x_proj.shape[0] * heads
    x_cols = x_proj.shape[1] // heads
    bc_cols = b_proj.shape[1] // heads
    dtype = x_proj.dtype
    shapes = [
        (rows, x_cols),
        (rows, x_cols),
        (rows, bc_cols),
        (rows, bc_cols),
        (rows, dt_raw.shape[1]),
        (HALO, x_cols),
        (HALO, bc_cols),
        (HALO, bc_cols),
    ]
    return pl.pallas_call(
        functools.partial(entry_kernel, count, heads),
        out_shape=[jax.ShapeDtypeStruct(shape, dtype) for shape in shapes],
        in_specs=[pl.BlockSpec(memory_space=pl.ANY)] * 5,
        out_specs=[pl.BlockSpec(memory_space=pl.ANY)] * 5
        + [pl.BlockSpec(memory_space=pltpu.VMEM)] * 3,
        scratch_shapes=[
            pltpu.SemaphoreType.DMA((5, heads)),
            pltpu.SemaphoreType.DMA((5, heads)),
            pltpu.SemaphoreType.DMA((5,)),
            pltpu.SemaphoreType.DMA((3, heads)),
            pltpu.SemaphoreType.DMA((3,)),
        ],
        compiler_params=pltpu.CompilerParams(collective_id=0, has_side_effects=True),
        name="entry_exchange",
    )(x_proj, z_proj, b_proj, c_proj, dt_raw)


def conv_silu(value_ref, halo_ref, taps_ref, bias_ref, padded):
    tokens = value_ref.shape[0]
    taps = taps_ref.shape[0]
    padded[0:8, :] = halo_ref[HALO - 8 : HALO, :].astype(jnp.float32)
    padded[8 : 8 + tokens, :] = value_ref[...].astype(jnp.float32)
    total = bias_ref[...] + jnp.zeros(value_ref.shape, jnp.float32)
    for offset in range(taps):
        low = 8 - (taps - 1) + offset
        total = total + taps_ref[offset : offset + 1, :] * padded[low : low + tokens, :]
    return (total / (1.0 + jnp.exp(-total))).astype(jnp.bfloat16)


def local_kernel(
    x_ref,
    b_ref,
    c_ref,
    x_halo,
    b_halo,
    c_halo,
    x_taps,
    x_bias,
    b_taps,
    b_bias,
    c_taps,
    c_bias,
    step_t,
    cum_t,
    cum_c,
    skip_ref,
    y_ref,
    piece_ref,
    final_ref,
    c_out,
    x_pad,
    bc_pad,
    x_t,
    x_w,
    final,
):
    tokens, width = x_ref.shape
    heads = step_t.shape[0]
    blocks = tokens // SPAN
    x_conv = conv_silu(x_ref, x_halo, x_taps, x_bias, x_pad)
    b_conv = conv_silu(b_ref, b_halo, b_taps, b_bias, bc_pad)
    c_conv = conv_silu(c_ref, c_halo, c_taps, c_bias, bc_pad)
    c_out[...] = c_conv
    later = lax.broadcasted_iota(jnp.int32, (SPAN, SPAN), 0)
    earlier = lax.broadcasted_iota(jnp.int32, (SPAN, SPAN), 1)
    causal = later >= earlier
    for block in range(blocks):
        low = block * SPAN
        b_blk = b_conv[low : low + SPAN]
        c_blk = c_conv[low : low + SPAN]
        x_t[...] = x_conv[low : low + SPAN].astype(jnp.float32).T
        scores = lax.dot_general(c_blk, b_blk, NT, preferred_element_type=jnp.float32)
        for head in range(heads):
            rows = pl.ds(head * HEAD_DIM, HEAD_DIM)
            column = cum_c[0, low : low + SPAN, head : head + 1]
            row = cum_t[head : head + 1, low : low + SPAN]
            step = step_t[head : head + 1, low : low + SPAN]
            total = row[:, SPAN - 1 : SPAN]
            decays = jnp.exp(jnp.where(causal, column - row, -jnp.inf))
            mix = (decays * step * scores).astype(jnp.bfloat16)
            x_head = x_t[rows, :]
            product = lax.dot_general(
                x_head.astype(jnp.bfloat16), mix, NT, preferred_element_type=jnp.float32
            )
            y_ref[block, rows, :] = product + skip_ref[0, head : head + 1, :] * x_head
            x_w[rows, :] = (x_head * (step * jnp.exp(total - row))).astype(jnp.bfloat16)
        piece = jnp.dot(x_w[...], b_blk, preferred_element_type=jnp.float32)
        piece_ref[block] = piece
        if block == 0:
            final[...] = piece
        else:
            for head in range(heads):
                rows = pl.ds(head * HEAD_DIM, HEAD_DIM)
                decay = jnp.exp(cum_t[head : head + 1, low + SPAN - 1 : low + SPAN])
                final[rows, :] = decay * final[rows, :] + piece_ref[block, rows, :]
    final_ref[...] = final[...].astype(jnp.bfloat16)


def local_scan(x, b, c, halos, x_taps, x_bias, bc_taps, bc_bias, step_t, cum_t, cum_c, skip):
    tokens, x_cols = x.shape
    groups = b.shape[1] // STATE
    width = x_cols // groups
    heads = width // HEAD_DIM
    blocks = tokens // SPAN
    taps = x_taps.shape[0]

    def cols(rows, size):
        return pl.BlockSpec((rows, size), lambda g: (0, g))

    in_specs = [
        cols(tokens, width),
        cols(tokens, STATE),
        cols(tokens, STATE),
        cols(HALO, width),
        cols(HALO, STATE),
        cols(HALO, STATE),
        cols(taps, width),
        cols(1, width),
        cols(taps, STATE),
        cols(1, STATE),
        cols(taps, STATE),
        cols(1, STATE),
        pl.BlockSpec((heads, tokens), lambda g: (g, 0)),
        pl.BlockSpec((heads, tokens), lambda g: (g, 0)),
        pl.BlockSpec((1, tokens, heads), lambda g: (g, 0, 0)),
        pl.BlockSpec((1, heads, 1), lambda g: (g, 0, 0)),
    ]
    out_specs = [
        pl.BlockSpec((blocks, width, SPAN), lambda g: (0, g, 0)),
        pl.BlockSpec((blocks, width, STATE), lambda g: (0, g, 0)),
        pl.BlockSpec((width, STATE), lambda g: (g, 0)),
        cols(tokens, STATE),
    ]
    out_shape = [
        jax.ShapeDtypeStruct((blocks, x_cols, SPAN), jnp.float32),
        jax.ShapeDtypeStruct((blocks, x_cols, STATE), jnp.float32),
        jax.ShapeDtypeStruct((x_cols, STATE), jnp.bfloat16),
        jax.ShapeDtypeStruct((tokens, groups * STATE), jnp.bfloat16),
    ]
    return pl.pallas_call(
        local_kernel,
        grid=(groups,),
        in_specs=in_specs,
        out_specs=out_specs,
        out_shape=out_shape,
        scratch_shapes=[
            pltpu.VMEM((tokens + 8, width), jnp.float32),
            pltpu.VMEM((tokens + 8, STATE), jnp.float32),
            pltpu.VMEM((width, SPAN), jnp.float32),
            pltpu.VMEM((width, SPAN), jnp.bfloat16),
            pltpu.VMEM((width, STATE), jnp.float32),
        ],
        compiler_params=pltpu.CompilerParams(dimension_semantics=("arbitrary",)),
        cost_estimate=pl.CostEstimate(
            flops=20000000000, bytes_accessed=16000000, transcendentals=4000000
        ),
        name="local_scan",
    )(
        x,
        b,
        c,
        *halos,
        x_taps,
        x_bias[None],
        bc_taps[:, 0],
        bc_bias[0:1],
        bc_taps[:, 1],
        bc_bias[1:2],
        step_t,
        cum_t,
        cum_c,
        skip,
    )


def carry_kernel(start_ref, piece_ref, c_ref, cum_t, y_ref, z_ref, gain_ref, out_ref, running, y_t):
    tokens, width = z_ref.shape
    heads = cum_t.shape[0]
    blocks = tokens // SPAN
    running[...] = start_ref[...].astype(jnp.float32)
    for block in range(blocks):
        low = block * SPAN
        c_blk = c_ref[low : low + SPAN, :]
        carried = lax.dot_general(
            running[...].astype(jnp.bfloat16), c_blk, NT, preferred_element_type=jnp.float32
        )
        y_t[...] = carried
        for head in range(heads):
            rows = pl.ds(head * HEAD_DIM, HEAD_DIM)
            row = jnp.exp(cum_t[head : head + 1, low : low + SPAN])
            y_t[rows, :] = y_ref[block, rows, :] + y_t[rows, :] * row
            if block < blocks - 1:
                running[rows, :] = (
                    row[:, SPAN - 1 : SPAN] * running[rows, :] + piece_ref[block, rows, :]
                )
        gate = z_ref[low : low + SPAN, :].astype(jnp.float32)
        gated = y_t[...].T * (gate / (1.0 + jnp.exp(-gate)))
        mean = jnp.sum(gated * gated, axis=-1, keepdims=True) * (1.0 / width)
        normed = gated * lax.rsqrt(mean + 1.0)
        out_ref[low : low + SPAN, :] = (normed * gain_ref[...]).astype(jnp.bfloat16)


def carry_norm(start, pieces, c_conv, cum_t, y_t, z, gain):
    tokens, x_cols = z.shape
    groups = c_conv.shape[1] // STATE
    width = x_cols // groups
    heads = width // HEAD_DIM
    blocks = tokens // SPAN
    return pl.pallas_call(
        carry_kernel,
        grid=(groups,),
        in_specs=[
            pl.BlockSpec((width, STATE), lambda g: (g, 0)),
            pl.BlockSpec((blocks, width, STATE), lambda g: (0, g, 0)),
            pl.BlockSpec((tokens, STATE), lambda g: (0, g)),
            pl.BlockSpec((heads, tokens), lambda g: (g, 0)),
            pl.BlockSpec((blocks, width, SPAN), lambda g: (0, g, 0)),
            pl.BlockSpec((tokens, width), lambda g: (0, g)),
            pl.BlockSpec((1, width), lambda g: (0, g)),
        ],
        out_specs=pl.BlockSpec((tokens, width), lambda g: (0, g)),
        out_shape=jax.ShapeDtypeStruct((tokens, x_cols), jnp.bfloat16),
        scratch_shapes=[
            pltpu.VMEM((width, STATE), jnp.float32),
            pltpu.VMEM((width, SPAN), jnp.float32),
        ],
        compiler_params=pltpu.CompilerParams(dimension_semantics=("arbitrary",)),
        cost_estimate=pl.CostEstimate(
            flops=5000000000, bytes_accessed=14000000, transcendentals=1000000
        ),
        name="carry_norm",
    )(start, pieces, c_conv, cum_t, y_t, z, gain[None])


def prefix_kernel(count, final_ref, logs_ref, out_ref, pieces, logs, starts, *sems):
    piece_send, piece_recv, log_send, log_recv, start_send, start_recv, own = sems
    seq = lax.axis_index("seq")
    head = lax.axis_index("head")
    rows = pieces.shape[1]
    barrier = pltpu.get_barrier_semaphore()

    def peer_of(step):
        return lax.rem(seq + step, count)

    def part(which):
        return pl.ds(pl.multiple_of(which * rows, 16), rows)

    def remote(source, target, send, recv, peer):
        return pltpu.make_async_remote_copy(
            src_ref=source,
            dst_ref=target,
            send_sem=send,
            recv_sem=recv,
            device_id=(peer, head),
            device_id_type=pl.DeviceIdType.MESH,
        )

    def log_copy(step):
        return remote(
            logs_ref, logs.at[seq], log_send.at[step], log_recv.at[step], peer_of(step)
        )

    def piece_copy(step):
        return remote(
            final_ref.at[part(peer_of(step))],
            pieces.at[seq],
            piece_send.at[step],
            piece_recv.at[step],
            peer_of(step),
        )

    def start_copy(step):
        return remote(
            starts.at[peer_of(step)],
            out_ref.at[part(seq)],
            start_send.at[step],
            start_recv.at[step],
            peer_of(step),
        )

    def each(body):
        def lap(step, carry):
            body(step)
            return carry

        lax.fori_loop(1, count, lap, 0)

    def greet(step):
        pl.semaphore_signal(
            barrier, inc=1, device_id=(peer_of(step), head), device_id_type=pl.DeviceIdType.MESH
        )

    each(greet)
    pl.semaphore_wait(barrier, count - 1)

    def send(step):
        log_copy(step).start()
        piece_copy(step).start()

    each(send)
    own_piece = pltpu.make_async_copy(final_ref.at[part(seq)], pieces.at[seq], own.at[0])
    own_log = pltpu.make_async_copy(logs_ref, logs.at[seq], own.at[1])
    own_piece.start()
    own_log.start()
    own_piece.wait()
    own_log.wait()

    def land(step):
        log_copy(step).wait()
        piece_copy(step).wait()

    each(land)
    per_head = min(rows, HEAD_DIM)
    first = seq * rows // HEAD_DIM
    lanes = logs.shape[2]

    def scan(position, running):
        for index in range(rows // per_head):
            low = index * per_head
            starts[position, low : low + per_head, :] = running[index].astype(jnp.bfloat16)
        decays = jnp.exp(pltpu.roll(logs[position], lax.rem(lanes - first, lanes), 1))
        following = []
        for index in range(rows // per_head):
            low = index * per_head
            piece = pieces[position, low : low + per_head, :].astype(jnp.float32)
            following.append(decays[0:1, index : index + 1] * running[index] + piece)
        return tuple(following)

    zero = jnp.zeros((per_head, pieces.shape[2]), jnp.float32)
    lax.fori_loop(0, count, scan, (zero,) * (rows // per_head))
    each(lambda step: start_copy(step).start())
    own_start = pltpu.make_async_copy(starts.at[seq], out_ref.at[part(seq)], own.at[0])
    own_start.start()
    own_start.wait()
    each(lambda step: start_copy(step).wait())


def carry_in(log_total, final_state):
    count = lax.axis_size("seq")
    total, width = final_state.shape
    rows = total // count
    logs = jnp.broadcast_to(jnp.pad(log_total, (0, 128 - log_total.shape[0]))[None], (8, 128))
    vmem = pl.BlockSpec(memory_space=pltpu.VMEM)
    dma = pltpu.SemaphoreType.DMA
    return pl.pallas_call(
        functools.partial(prefix_kernel, count),
        out_shape=jax.ShapeDtypeStruct(final_state.shape, final_state.dtype),
        in_specs=[vmem, vmem],
        out_specs=vmem,
        scratch_shapes=[
            pltpu.VMEM((count, rows, width), jnp.bfloat16),
            pltpu.VMEM((count, 8, 128), jnp.float32),
            pltpu.VMEM((count, rows, width), jnp.bfloat16),
            dma((count,)),
            dma((count,)),
            dma((count,)),
            dma((count,)),
            dma((count,)),
            dma((count,)),
            dma((2,)),
        ],
        compiler_params=pltpu.CompilerParams(collective_id=1, has_side_effects=True),
        name="prefix_exchange",
    )(final_state, logs)


def project_kernel(
    heads, normed, weight, out, buffer, terms, landed, load_sems, send_sems, recv_sems
):
    seq = lax.axis_index("seq")
    head = lax.axis_index("head")
    rows = out.shape[0]
    tile = buffer.shape[2]
    tiles = out.shape[1] // tile
    barrier = pltpu.get_barrier_semaphore()
    for step in range(1, heads):
        pl.semaphore_signal(
            barrier,
            inc=1,
            device_id=(seq, lax.rem(head + step, heads)),
            device_id_type=pl.DeviceIdType.MESH,
        )
    pl.semaphore_wait(barrier, heads - 1)

    def load(index):
        slot = lax.rem(index, 2)
        return pltpu.make_async_copy(
            weight.at[:, pl.ds(pl.multiple_of(index * tile, 128), tile)],
            buffer.at[slot],
            load_sems.at[slot],
        )

    def share(index, step):
        peer = lax.rem(head + step, heads)
        return pltpu.make_async_remote_copy(
            src_ref=terms.at[index, pl.ds(pl.multiple_of(peer * rows, 16), rows)],
            dst_ref=landed.at[index, step - 1],
            send_sem=send_sems.at[index, step - 1],
            recv_sem=recv_sems.at[index, step - 1],
            device_id=(seq, peer),
            device_id_type=pl.DeviceIdType.MESH,
        )

    load(0).start()

    def multiply(index, carry):
        @pl.when(index + 1 < tiles)
        def _():
            load(index + 1).start()

        load(index).wait()
        product = jnp.dot(
            normed[...], buffer[lax.rem(index, 2)], preferred_element_type=jnp.float32
        )
        terms[index] = product.astype(jnp.bfloat16)
        for step in range(1, heads):
            share(index, step).start()
        return carry

    lax.fori_loop(0, tiles, multiply, 0)
    for index in range(tiles):
        own = terms[index, pl.ds(pl.multiple_of(head * rows, 16), rows), :]
        total = own.astype(jnp.float32)
        for step in range(1, heads):
            share(index, step).wait()
            total = total + landed[index, step - 1].astype(jnp.float32)
        out[:, index * tile : (index + 1) * tile] = total.astype(jnp.bfloat16)


def project(normed, weight):
    heads = lax.axis_size("head")
    tokens, depth = normed.shape
    columns = weight.shape[1]
    rows = tokens // heads
    tile = min(columns, 256)
    tiles = columns // tile
    dma = pltpu.SemaphoreType.DMA
    return pl.pallas_call(
        functools.partial(project_kernel, heads),
        out_shape=jax.ShapeDtypeStruct((rows, columns), jnp.bfloat16),
        in_specs=[
            pl.BlockSpec(memory_space=pltpu.VMEM),
            pl.BlockSpec(memory_space=pl.ANY),
        ],
        out_specs=pl.BlockSpec(memory_space=pltpu.VMEM),
        scratch_shapes=[
            pltpu.VMEM((2, depth, tile), jnp.bfloat16),
            pltpu.VMEM((tiles, tokens, tile), jnp.bfloat16),
            pltpu.VMEM((tiles, heads - 1, rows, tile), jnp.bfloat16),
            dma((2,)),
            dma((tiles, heads - 1)),
            dma((tiles, heads - 1)),
        ],
        compiler_params=pltpu.CompilerParams(collective_id=2, has_side_effects=True),
        cost_estimate=pl.CostEstimate(
            flops=2 * tokens * depth * columns,
            bytes_accessed=2 * depth * columns,
            transcendentals=0,
        ),
        name="project",
    )(normed, weight)


def per_device(
    x_proj,
    z_proj,
    b_proj,
    c_proj,
    dt_raw,
    dt_bias,
    a_log,
    d_skip,
    conv_x,
    conv_bias_x,
    conv_bc,
    conv_bias_bc,
    norm_weight,
    out_weight,
):
    x_heads, z_heads, b_heads, c_heads, dt_full, *halos = entry_exchange(
        x_proj, z_proj, b_proj, c_proj, dt_raw
    )
    token_count = x_heads.shape[0]
    local_heads = dt_bias.shape[0]
    local_groups = b_heads.shape[1] // STATE
    per_group = local_heads // local_groups
    blocks = token_count // SPAN
    dt_heads = lax.dynamic_slice_in_dim(
        dt_full, lax.axis_index("head") * local_heads, local_heads, axis=1
    )
    step_size = jax.nn.softplus(dt_heads.astype(jnp.float32) + dt_bias)
    rate = (-jnp.exp(a_log) * step_size).reshape(blocks, SPAN, local_heads)
    cumulative = jnp.cumsum(rate, axis=1)
    log_total = jnp.sum(cumulative[:, -1], axis=0)
    cumulative = cumulative.reshape(token_count, local_heads)
    step_t = step_size.T
    cum_t = cumulative.T
    cum_c = jnp.transpose(
        cumulative.reshape(token_count, local_groups, per_group), (1, 0, 2)
    )
    y_t, pieces, final_state, c_conv = local_scan(
        x_heads,
        b_heads,
        c_heads,
        halos,
        conv_x,
        conv_bias_x,
        conv_bc,
        conv_bias_bc,
        step_t,
        cum_t,
        cum_c,
        d_skip.reshape(local_groups, per_group, 1),
    )
    start = carry_in(log_total, final_state)
    normed = carry_norm(start, pieces, c_conv, cum_t, y_t, z_heads, norm_weight)
    weight = lax.all_gather(out_weight, "seq", axis=1, tiled=True)
    return project(normed, weight)


def solution(mesh):
    in_specs = (
        P(("seq", "head"), None),
        P(("seq", "head"), None),
        P(("seq", "head"), None),
        P(("seq", "head"), None),
        P(("seq", "head"), None),
        P("head"),
        P("head"),
        P("head"),
        P(None, "head"),
        P("head"),
        P(None, None, "head"),
        P(None, "head"),
        P("head"),
        P("head", "seq"),
    )
    out_specs = P(("seq", "head"), None)
    return jax.shard_map(
        per_device, mesh=mesh, in_specs=in_specs, out_specs=out_specs, check_vma=False
    )
```

```python
import functools

import jax
import jax.numpy as jnp
from jax import lax
from jax.experimental import pallas as pl
from jax.experimental.pallas import tpu as pltpu
from jax.sharding import PartitionSpec as P

HEAD_DIM = 64
STATE = 128
GROUPS = 8
SPAN = 128
DI = 8192
HALO = 16
NT = (((1,), (1,)), ((), ()))


def entry_kernel(count, heads, *refs):
    x_in, z_in, b_in, c_in, dt_in = refs[:5]
    x_out, z_out, b_out, c_out, dt_out, x_halo, b_halo, c_halo = refs[5:13]
    send_sems, recv_sems, local_sems, halo_send, halo_recv = refs[13:]
    seq = lax.axis_index("seq")
    head = lax.axis_index("head")
    rows = x_in.shape[0]
    barrier = pltpu.get_barrier_semaphore()
    last_head = head == heads - 1
    gives_halo = jnp.logical_and(last_head, seq < count - 1)
    takes_halo = seq > 0
    for step in range(1, heads):
        peer = lax.rem(head + step, heads)
        pl.semaphore_signal(
            barrier, inc=1, device_id=(seq, peer), device_id_type=pl.DeviceIdType.MESH
        )

    @pl.when(takes_halo)
    def _():
        pl.semaphore_signal(
            barrier,
            inc=1,
            device_id=(seq - 1, heads - 1),
            device_id_type=pl.DeviceIdType.MESH,
        )

    pl.semaphore_wait(barrier, heads - 1 + jnp.where(gives_halo, heads, 0))

    def columns(ref, width, which):
        return ref.at[:, pl.ds(pl.multiple_of(which * width, 128), width)]

    mine = pl.ds(pl.multiple_of(head * rows, 16), rows)
    plan = (
        (b_in, b_out, True),
        (c_in, c_out, True),
        (dt_in, dt_out, False),
        (x_in, x_out, True),
        (z_in, z_out, True),
    )
    halos = ((x_in, x_halo), (b_in, b_halo), (c_in, c_halo))

    def halo_copy(index, peer):
        source, target = halos[index]
        width = target.shape[1]
        return pltpu.make_async_remote_copy(
            src_ref=source.at[pl.ds(rows - HALO, HALO), pl.ds(peer * width, width)],
            dst_ref=target,
            send_sem=halo_send.at[index, peer],
            recv_sem=halo_recv.at[index],
            device_id=(seq + 1, peer),
            device_id_type=pl.DeviceIdType.MESH,
        )

    @pl.when(gives_halo)
    def _():
        for index in range(len(halos)):
            for peer in range(heads):
                halo_copy(index, peer).start()

    copies = []
    for step in range(1, heads):
        peer = lax.rem(head + step, heads)
        for index, (source, target, split) in enumerate(plan):
            view = columns(source, target.shape[1], peer) if split else source
            copy = pltpu.make_async_remote_copy(
                src_ref=view,
                dst_ref=target.at[mine],
                send_sem=send_sems.at[index, step],
                recv_sem=recv_sems.at[index, step],
                device_id=(seq, peer),
                device_id_type=pl.DeviceIdType.MESH,
            )
            copy.start()
            copies.append(copy)
    for index, (source, target, split) in enumerate(plan):
        view = columns(source, target.shape[1], head) if split else source
        copy = pltpu.make_async_copy(view, target.at[mine], local_sems.at[index])
        copy.start()
        copies.append(copy)

    @pl.when(jnp.logical_not(takes_halo))
    def _():
        for _, target in halos:
            target[...] = jnp.zeros_like(target)

    @pl.when(takes_halo)
    def _():
        for index, (source, target) in enumerate(halos):
            pltpu.make_async_remote_copy(
                src_ref=source.at[pl.ds(rows - HALO, HALO), pl.ds(0, target.shape[1])],
                dst_ref=target,
                send_sem=halo_send.at[index, 0],
                recv_sem=halo_recv.at[index],
                device_id=(seq, head),
                device_id_type=pl.DeviceIdType.MESH,
            ).wait_recv()

    @pl.when(gives_halo)
    def _():
        for index in range(len(halos)):
            for peer in range(heads):
                halo_copy(index, peer).wait_send()

    for copy in copies:
        copy.wait()


def entry_exchange(x_proj, z_proj, b_proj, c_proj, dt_raw):
    count = lax.axis_size("seq")
    heads = lax.axis_size("head")
    rows = x_proj.shape[0] * heads
    x_cols = x_proj.shape[1] // heads
    bc_cols = b_proj.shape[1] // heads
    dtype = x_proj.dtype
    shapes = [
        (rows, x_cols),
        (rows, x_cols),
        (rows, bc_cols),
        (rows, bc_cols),
        (rows, dt_raw.shape[1]),
        (HALO, x_cols),
        (HALO, bc_cols),
        (HALO, bc_cols),
    ]
    return pl.pallas_call(
        functools.partial(entry_kernel, count, heads),
        out_shape=[jax.ShapeDtypeStruct(shape, dtype) for shape in shapes],
        in_specs=[pl.BlockSpec(memory_space=pl.ANY)] * 5,
        out_specs=[pl.BlockSpec(memory_space=pl.ANY)] * 5
        + [pl.BlockSpec(memory_space=pltpu.VMEM)] * 3,
        scratch_shapes=[
            pltpu.SemaphoreType.DMA((5, heads)),
            pltpu.SemaphoreType.DMA((5, heads)),
            pltpu.SemaphoreType.DMA((5,)),
            pltpu.SemaphoreType.DMA((3, heads)),
            pltpu.SemaphoreType.DMA((3,)),
        ],
        compiler_params=pltpu.CompilerParams(collective_id=0, has_side_effects=True),
        name="entry_exchange",
    )(x_proj, z_proj, b_proj, c_proj, dt_raw)


def conv_silu(value_ref, halo_ref, taps_ref, bias_ref, padded):
    tokens = value_ref.shape[0]
    taps = taps_ref.shape[0]
    padded[0:8, :] = halo_ref[HALO - 8 : HALO, :].astype(jnp.float32)
    padded[8 : 8 + tokens, :] = value_ref[...].astype(jnp.float32)
    total = bias_ref[...] + jnp.zeros(value_ref.shape, jnp.float32)
    for offset in range(taps):
        low = 8 - (taps - 1) + offset
        total = total + taps_ref[offset : offset + 1, :] * padded[low : low + tokens, :]
    return (total / (1.0 + jnp.exp(-total))).astype(jnp.bfloat16)


def local_kernel(
    x_ref,
    b_ref,
    c_ref,
    x_halo,
    b_halo,
    c_halo,
    x_taps,
    x_bias,
    b_taps,
    b_bias,
    c_taps,
    c_bias,
    step_t,
    cum_t,
    cum_c,
    skip_ref,
    y_ref,
    piece_ref,
    final_ref,
    c_out,
    x_pad,
    bc_pad,
    x_t,
    x_w,
    final,
):
    tokens, width = x_ref.shape
    heads = step_t.shape[0]
    blocks = tokens // SPAN
    x_conv = conv_silu(x_ref, x_halo, x_taps, x_bias, x_pad)
    b_conv = conv_silu(b_ref, b_halo, b_taps, b_bias, bc_pad)
    c_conv = conv_silu(c_ref, c_halo, c_taps, c_bias, bc_pad)
    c_out[...] = c_conv
    later = lax.broadcasted_iota(jnp.int32, (SPAN, SPAN), 0)
    earlier = lax.broadcasted_iota(jnp.int32, (SPAN, SPAN), 1)
    causal = later >= earlier
    for block in range(blocks):
        low = block * SPAN
        b_blk = b_conv[low : low + SPAN]
        c_blk = c_conv[low : low + SPAN]
        x_t[...] = x_conv[low : low + SPAN].astype(jnp.float32).T
        scores = lax.dot_general(c_blk, b_blk, NT, preferred_element_type=jnp.float32)
        for head in range(heads):
            rows = pl.ds(head * HEAD_DIM, HEAD_DIM)
            column = cum_c[0, low : low + SPAN, head : head + 1]
            row = cum_t[head : head + 1, low : low + SPAN]
            step = step_t[head : head + 1, low : low + SPAN]
            total = row[:, SPAN - 1 : SPAN]
            decays = jnp.exp(jnp.where(causal, column - row, -jnp.inf))
            mix = (decays * step * scores).astype(jnp.bfloat16)
            x_head = x_t[rows, :]
            product = lax.dot_general(
                x_head.astype(jnp.bfloat16), mix, NT, preferred_element_type=jnp.float32
            )
            y_ref[block, rows, :] = product + skip_ref[0, head : head + 1, :] * x_head
            x_w[rows, :] = (x_head * (step * jnp.exp(total - row))).astype(jnp.bfloat16)
        piece = jnp.dot(x_w[...], b_blk, preferred_element_type=jnp.float32)
        piece_ref[block] = piece
        if block == 0:
            final[...] = piece
        else:
            for head in range(heads):
                rows = pl.ds(head * HEAD_DIM, HEAD_DIM)
                decay = jnp.exp(cum_t[head : head + 1, low + SPAN - 1 : low + SPAN])
                final[rows, :] = decay * final[rows, :] + piece_ref[block, rows, :]
    final_ref[...] = final[...].astype(jnp.bfloat16)


def local_scan(x, b, c, halos, x_taps, x_bias, bc_taps, bc_bias, step_t, cum_t, cum_c, skip):
    tokens, x_cols = x.shape
    groups = b.shape[1] // STATE
    width = x_cols // groups
    heads = width // HEAD_DIM
    blocks = tokens // SPAN
    taps = x_taps.shape[0]

    def cols(rows, size):
        return pl.BlockSpec((rows, size), lambda g: (0, g))

    in_specs = [
        cols(tokens, width),
        cols(tokens, STATE),
        cols(tokens, STATE),
        cols(HALO, width),
        cols(HALO, STATE),
        cols(HALO, STATE),
        cols(taps, width),
        cols(1, width),
        cols(taps, STATE),
        cols(1, STATE),
        cols(taps, STATE),
        cols(1, STATE),
        pl.BlockSpec((heads, tokens), lambda g: (g, 0)),
        pl.BlockSpec((heads, tokens), lambda g: (g, 0)),
        pl.BlockSpec((1, tokens, heads), lambda g: (g, 0, 0)),
        pl.BlockSpec((1, heads, 1), lambda g: (g, 0, 0)),
    ]
    out_specs = [
        pl.BlockSpec((blocks, width, SPAN), lambda g: (0, g, 0)),
        pl.BlockSpec((blocks, width, STATE), lambda g: (0, g, 0)),
        pl.BlockSpec((width, STATE), lambda g: (g, 0)),
        cols(tokens, STATE),
    ]
    out_shape = [
        jax.ShapeDtypeStruct((blocks, x_cols, SPAN), jnp.float32),
        jax.ShapeDtypeStruct((blocks, x_cols, STATE), jnp.float32),
        jax.ShapeDtypeStruct((x_cols, STATE), jnp.bfloat16),
        jax.ShapeDtypeStruct((tokens, groups * STATE), jnp.bfloat16),
    ]
    return pl.pallas_call(
        local_kernel,
        grid=(groups,),
        in_specs=in_specs,
        out_specs=out_specs,
        out_shape=out_shape,
        scratch_shapes=[
            pltpu.VMEM((tokens + 8, width), jnp.float32),
            pltpu.VMEM((tokens + 8, STATE), jnp.float32),
            pltpu.VMEM((width, SPAN), jnp.float32),
            pltpu.VMEM((width, SPAN), jnp.bfloat16),
            pltpu.VMEM((width, STATE), jnp.float32),
        ],
        compiler_params=pltpu.CompilerParams(dimension_semantics=("arbitrary",)),
        cost_estimate=pl.CostEstimate(
            flops=20000000000, bytes_accessed=16000000, transcendentals=4000000
        ),
        name="local_scan",
    )(
        x,
        b,
        c,
        *halos,
        x_taps,
        x_bias[None],
        bc_taps[:, 0],
        bc_bias[0:1],
        bc_taps[:, 1],
        bc_bias[1:2],
        step_t,
        cum_t,
        cum_c,
        skip,
    )


def carry_kernel(start_ref, piece_ref, c_ref, cum_t, y_ref, z_ref, gain_ref, out_ref, running, y_t):
    tokens, width = z_ref.shape
    heads = cum_t.shape[0]
    blocks = tokens // SPAN
    running[...] = start_ref[...].astype(jnp.float32)
    for block in range(blocks):
        low = block * SPAN
        c_blk = c_ref[low : low + SPAN, :]
        carried = lax.dot_general(
            running[...].astype(jnp.bfloat16), c_blk, NT, preferred_element_type=jnp.float32
        )
        y_t[...] = carried
        for head in range(heads):
            rows = pl.ds(head * HEAD_DIM, HEAD_DIM)
            row = jnp.exp(cum_t[head : head + 1, low : low + SPAN])
            y_t[rows, :] = y_ref[block, rows, :] + y_t[rows, :] * row
            if block < blocks - 1:
                running[rows, :] = (
                    row[:, SPAN - 1 : SPAN] * running[rows, :] + piece_ref[block, rows, :]
                )
        gate = z_ref[low : low + SPAN, :].astype(jnp.float32)
        gated = y_t[...].T * (gate / (1.0 + jnp.exp(-gate)))
        mean = jnp.sum(gated * gated, axis=-1, keepdims=True) * (1.0 / width)
        normed = gated * lax.rsqrt(mean + 1.0)
        out_ref[low : low + SPAN, :] = (normed * gain_ref[...]).astype(jnp.bfloat16)


def carry_norm(start, pieces, c_conv, cum_t, y_t, z, gain):
    tokens, x_cols = z.shape
    groups = c_conv.shape[1] // STATE
    width = x_cols // groups
    heads = width // HEAD_DIM
    blocks = tokens // SPAN
    return pl.pallas_call(
        carry_kernel,
        grid=(groups,),
        in_specs=[
            pl.BlockSpec((width, STATE), lambda g: (g, 0)),
            pl.BlockSpec((blocks, width, STATE), lambda g: (0, g, 0)),
            pl.BlockSpec((tokens, STATE), lambda g: (0, g)),
            pl.BlockSpec((heads, tokens), lambda g: (g, 0)),
            pl.BlockSpec((blocks, width, SPAN), lambda g: (0, g, 0)),
            pl.BlockSpec((tokens, width), lambda g: (0, g)),
            pl.BlockSpec((1, width), lambda g: (0, g)),
        ],
        out_specs=pl.BlockSpec((tokens, width), lambda g: (0, g)),
        out_shape=jax.ShapeDtypeStruct((tokens, x_cols), jnp.bfloat16),
        scratch_shapes=[
            pltpu.VMEM((width, STATE), jnp.float32),
            pltpu.VMEM((width, SPAN), jnp.float32),
        ],
        compiler_params=pltpu.CompilerParams(dimension_semantics=("arbitrary",)),
        cost_estimate=pl.CostEstimate(
            flops=5000000000, bytes_accessed=14000000, transcendentals=1000000
        ),
        name="carry_norm",
    )(start, pieces, c_conv, cum_t, y_t, z, gain[None])


def prefix_kernel(count, final_ref, logs_ref, out_ref, pieces, logs, starts, *sems):
    piece_send, piece_recv, log_send, log_recv, start_send, start_recv, own = sems
    seq = lax.axis_index("seq")
    head = lax.axis_index("head")
    rows = pieces.shape[1]
    barrier = pltpu.get_barrier_semaphore()

    def peer_of(step):
        return lax.rem(seq + step, count)

    def part(which):
        return pl.ds(pl.multiple_of(which * rows, 16), rows)

    def remote(source, target, send, recv, peer):
        return pltpu.make_async_remote_copy(
            src_ref=source,
            dst_ref=target,
            send_sem=send,
            recv_sem=recv,
            device_id=(peer, head),
            device_id_type=pl.DeviceIdType.MESH,
        )

    def log_copy(step):
        return remote(
            logs_ref, logs.at[seq], log_send.at[step], log_recv.at[step], peer_of(step)
        )

    def piece_copy(step):
        return remote(
            final_ref.at[part(peer_of(step))],
            pieces.at[seq],
            piece_send.at[step],
            piece_recv.at[step],
            peer_of(step),
        )

    def start_copy(step):
        return remote(
            starts.at[peer_of(step)],
            out_ref.at[part(seq)],
            start_send.at[step],
            start_recv.at[step],
            peer_of(step),
        )

    def each(body):
        def lap(step, carry):
            body(step)
            return carry

        lax.fori_loop(1, count, lap, 0)

    def greet(step):
        pl.semaphore_signal(
            barrier, inc=1, device_id=(peer_of(step), head), device_id_type=pl.DeviceIdType.MESH
        )

    each(greet)
    pl.semaphore_wait(barrier, count - 1)

    def send(step):
        log_copy(step).start()
        piece_copy(step).start()

    each(send)
    own_piece = pltpu.make_async_copy(final_ref.at[part(seq)], pieces.at[seq], own.at[0])
    own_log = pltpu.make_async_copy(logs_ref, logs.at[seq], own.at[1])
    own_piece.start()
    own_log.start()
    own_piece.wait()
    own_log.wait()

    def land(step):
        log_copy(step).wait()
        piece_copy(step).wait()

    each(land)
    per_head = min(rows, HEAD_DIM)
    first = seq * rows // HEAD_DIM
    lanes = logs.shape[2]

    def scan(position, running):
        for index in range(rows // per_head):
            low = index * per_head
            starts[position, low : low + per_head, :] = running[index].astype(jnp.bfloat16)
        decays = jnp.exp(pltpu.roll(logs[position], lax.rem(lanes - first, lanes), 1))
        following = []
        for index in range(rows // per_head):
            low = index * per_head
            piece = pieces[position, low : low + per_head, :].astype(jnp.float32)
            following.append(decays[0:1, index : index + 1] * running[index] + piece)
        return tuple(following)

    zero = jnp.zeros((per_head, pieces.shape[2]), jnp.float32)
    lax.fori_loop(0, count, scan, (zero,) * (rows // per_head))
    each(lambda step: start_copy(step).start())
    own_start = pltpu.make_async_copy(starts.at[seq], out_ref.at[part(seq)], own.at[0])
    own_start.start()
    own_start.wait()
    each(lambda step: start_copy(step).wait())


def carry_in(log_total, final_state):
    count = lax.axis_size("seq")
    total, width = final_state.shape
    rows = total // count
    logs = jnp.broadcast_to(jnp.pad(log_total, (0, 128 - log_total.shape[0]))[None], (8, 128))
    vmem = pl.BlockSpec(memory_space=pltpu.VMEM)
    dma = pltpu.SemaphoreType.DMA
    return pl.pallas_call(
        functools.partial(prefix_kernel, count),
        out_shape=jax.ShapeDtypeStruct(final_state.shape, final_state.dtype),
        in_specs=[vmem, vmem],
        out_specs=vmem,
        scratch_shapes=[
            pltpu.VMEM((count, rows, width), jnp.bfloat16),
            pltpu.VMEM((count, 8, 128), jnp.float32),
            pltpu.VMEM((count, rows, width), jnp.bfloat16),
            dma((count,)),
            dma((count,)),
            dma((count,)),
            dma((count,)),
            dma((count,)),
            dma((count,)),
            dma((2,)),
        ],
        compiler_params=pltpu.CompilerParams(collective_id=1, has_side_effects=True),
        name="prefix_exchange",
    )(final_state, logs)


def project_kernel(
    heads, normed, weight, out, buffer, terms, landed, load_sems, send_sems, recv_sems
):
    seq = lax.axis_index("seq")
    head = lax.axis_index("head")
    rows = out.shape[0]
    tile = buffer.shape[2]
    tiles = out.shape[1] // tile
    barrier = pltpu.get_barrier_semaphore()
    for step in range(1, heads):
        pl.semaphore_signal(
            barrier,
            inc=1,
            device_id=(seq, lax.rem(head + step, heads)),
            device_id_type=pl.DeviceIdType.MESH,
        )
    pl.semaphore_wait(barrier, heads - 1)

    def load(index):
        slot = lax.rem(index, 2)
        return pltpu.make_async_copy(
            weight.at[index],
            buffer.at[slot],
            load_sems.at[slot],
        )

    def share(index, step):
        peer = lax.rem(head + step, heads)
        return pltpu.make_async_remote_copy(
            src_ref=terms.at[index, pl.ds(pl.multiple_of(peer * rows, 16), rows)],
            dst_ref=landed.at[index, step - 1],
            send_sem=send_sems.at[index, step - 1],
            recv_sem=recv_sems.at[index, step - 1],
            device_id=(seq, peer),
            device_id_type=pl.DeviceIdType.MESH,
        )

    load(0).start()

    def multiply(index, carry):
        @pl.when(index + 1 < tiles)
        def _():
            load(index + 1).start()

        load(index).wait()
        product = jnp.dot(
            normed[...], buffer[lax.rem(index, 2)], preferred_element_type=jnp.float32
        )
        terms[index] = product.astype(jnp.bfloat16)
        for step in range(1, heads):
            share(index, step).start()
        return carry

    lax.fori_loop(0, tiles, multiply, 0)
    for index in range(tiles):
        own = terms[index, pl.ds(pl.multiple_of(head * rows, 16), rows), :]
        total = own.astype(jnp.float32)
        for step in range(1, heads):
            share(index, step).wait()
            total = total + landed[index, step - 1].astype(jnp.float32)
        out[:, index * tile : (index + 1) * tile] = total.astype(jnp.bfloat16)


def project(normed, weight):
    heads = lax.axis_size("head")
    tokens, depth = normed.shape
    tiles, _, tile = weight.shape
    columns = tiles * tile
    rows = tokens // heads
    dma = pltpu.SemaphoreType.DMA
    return pl.pallas_call(
        functools.partial(project_kernel, heads),
        out_shape=jax.ShapeDtypeStruct((rows, columns), jnp.bfloat16),
        in_specs=[
            pl.BlockSpec(memory_space=pltpu.VMEM),
            pl.BlockSpec(memory_space=pl.ANY),
        ],
        out_specs=pl.BlockSpec(memory_space=pltpu.VMEM),
        scratch_shapes=[
            pltpu.VMEM((2, depth, tile), jnp.bfloat16),
            pltpu.VMEM((tiles, tokens, tile), jnp.bfloat16),
            pltpu.VMEM((tiles, heads - 1, rows, tile), jnp.bfloat16),
            dma((2,)),
            dma((tiles, heads - 1)),
            dma((tiles, heads - 1)),
        ],
        compiler_params=pltpu.CompilerParams(collective_id=2, has_side_effects=True),
        cost_estimate=pl.CostEstimate(
            flops=2 * tokens * depth * columns,
            bytes_accessed=2 * depth * columns,
            transcendentals=0,
        ),
        name="project",
    )(normed, weight)


def per_device(
    x_proj,
    z_proj,
    b_proj,
    c_proj,
    dt_raw,
    dt_bias,
    a_log,
    d_skip,
    conv_x,
    conv_bias_x,
    conv_bc,
    conv_bias_bc,
    norm_weight,
    out_weight,
):
    x_heads, z_heads, b_heads, c_heads, dt_full, *halos = entry_exchange(
        x_proj, z_proj, b_proj, c_proj, dt_raw
    )
    token_count = x_heads.shape[0]
    local_heads = dt_bias.shape[0]
    local_groups = b_heads.shape[1] // STATE
    per_group = local_heads // local_groups
    blocks = token_count // SPAN
    dt_heads = lax.dynamic_slice_in_dim(
        dt_full, lax.axis_index("head") * local_heads, local_heads, axis=1
    )
    step_size = jax.nn.softplus(dt_heads.astype(jnp.float32) + dt_bias)
    rate = (-jnp.exp(a_log) * step_size).reshape(blocks, SPAN, local_heads)
    cumulative = jnp.cumsum(rate, axis=1)
    log_total = jnp.sum(cumulative[:, -1], axis=0)
    cumulative = cumulative.reshape(token_count, local_heads)
    step_t = step_size.T
    cum_t = cumulative.T
    cum_c = jnp.transpose(
        cumulative.reshape(token_count, local_groups, per_group), (1, 0, 2)
    )
    y_t, pieces, final_state, c_conv = local_scan(
        x_heads,
        b_heads,
        c_heads,
        halos,
        conv_x,
        conv_bias_x,
        conv_bc,
        conv_bias_bc,
        step_t,
        cum_t,
        cum_c,
        d_skip.reshape(local_groups, per_group, 1),
    )
    start = carry_in(log_total, final_state)
    normed = carry_norm(start, pieces, c_conv, cum_t, y_t, z_heads, norm_weight)
    weight = lax.all_gather(out_weight, "seq")
    return project(normed, weight)


def solution(mesh):
    in_specs = (
        P(("seq", "head"), None),
        P(("seq", "head"), None),
        P(("seq", "head"), None),
        P(("seq", "head"), None),
        P(("seq", "head"), None),
        P("head"),
        P("head"),
        P("head"),
        P(None, "head"),
        P("head"),
        P(None, None, "head"),
        P(None, "head"),
        P("head"),
        P("head", "seq"),
    )
    out_specs = P(("seq", "head"), None)
    return jax.shard_map(
        per_device, mesh=mesh, in_specs=in_specs, out_specs=out_specs, check_vma=False
    )
```
